32 devices in a mesh: tm: 16 (over z, y, x), space: 2 (over core).
Axes of the slice: x: 2, y: 2, z: 4, core: 2. Of those that a mesh axis runs over, the one named last changes fastest.
Arguments:
- initial: float32 [16, 32, 64, 128], P('tm', 'space'), may hold values from -6 to 6
- source: float32 [16, 32, 64, 128], P('tm', 'space'), may hold values from -6 to 6
- diffusion: float32 [32, 64, 128], P('space'), may hold values from 0.1 to 1
- advection: float32 [3, 32, 64, 128], P(None, 'space'), may hold values from 0.05 to 0.5
Outputs:
- smoothed: float32 [16, 32, 64, 128], P('tm', 'space')
- residual: float32 [16, 32, 64, 128], P('tm', 'space')
The draws below stay inside these ranges and needn't reach their ends.
All inputs are finite; a program needn't handle non-finite values.
Results may differ from the reference program's by a relative error of at most 0.00002.
Values sent between devices are 32-bit elements; how exact they have to be, the bound alone decides.
A program may use at most 64 MiB of HBM per device.

```python
import math
import jax
import jax.numpy as jnp

SWEEPS = 2
ITERS = 4
NX = 64
NY = 128
NT = 16
NZ = 32


def level_of(stream_key, dims, pieces, smallest, top_value):
    def one(position, shards_of):
        draws = jax.random.uniform(jax.random.fold_in(jax.random.fold_in(stream_key, 6), position), (shards_of,), jnp.float32, smallest / len(pieces), top_value / len(pieces))
        return jnp.repeat(jnp.exp(draws), dims[position] // shards_of).reshape((-1,) + (1,) * (len(dims) - position - 1))

    level = one(*pieces[0])
    for cut in pieces[1:]:
        level = level * one(*cut)
    return level


def normal_values(own_key, shape, deviation, most, shards=(), kind=jnp.bfloat16):
    drawn = jax.random.normal(own_key, shape, jnp.float32) * deviation
    if len(shards) > 0:
        drawn = level_of(own_key, shape, shards, -0.22, 0.18) * drawn
    return jnp.clip(drawn, min=-most, max=most).astype(kind)


def setup_inputs(seed: int = 0) -> dict:
    seeds = jax.random.split(jax.random.key(seed), 5)
    initial = normal_values(seeds[0], (NT, NZ, NX, NY), 1.0, 6.0, ((0, 16), (1, 2)), jnp.float32)
    source = normal_values(seeds[1], (NT, NZ, NX, NY), 1.0, 6.0, ((0, 16), (1, 2)), jnp.float32)
    diffusion = jnp.clip(jnp.exp(math.log(1.0) - 2.3025851 * jax.random.uniform(seeds[2], (NZ, NX, NY), jnp.float32) ** level_of(seeds[2], (NZ, NX, NY), ((0, 2),), -0.2, 0.2)), 0.1, 1.0)
    advection = jnp.clip(jnp.exp(math.log(0.5) - 2.3025851 * jax.random.uniform(seeds[3], (3, NZ, NX, NY), jnp.float32) ** level_of(seeds[3], (3, NZ, NX, NY), ((1, 2),), -0.2, 0.2)), 0.05, 0.5)
    return {"initial": initial, "source": source, "diffusion": diffusion, "advection": advection}


def off_terms(padded, spread, upwind):
    low_z = padded[..., :-2, 1:-1, 1:-1]
    high_z = padded[..., 2:, 1:-1, 1:-1]
    low_x = padded[..., 1:-1, :-2, 1:-1]
    high_x = padded[..., 1:-1, 2:, 1:-1]
    low_y = padded[..., 1:-1, 1:-1, :-2]
    high_y = padded[..., 1:-1, 1:-1, 2:]
    total = spread * (high_z + low_z + high_x + low_x + high_y + low_y)
    return total + upwind[0] * low_x + upwind[1] * low_y + upwind[2] * low_z


def main_diagonal(spread, upwind):
    return 1.0 + 6.0 * spread + (upwind[0] + upwind[1] + upwind[2])


def pad_space(field):
    return jnp.pad(field, ((0, 0), (1, 1), (1, 1), (1, 1)))


def reference(initial, source, diffusion, advection):
    diagonal = main_diagonal(diffusion, advection)
    smoothed = initial
    for sweep in range(SWEEPS):
        prior = jnp.roll(smoothed, 1, axis=0)
        forcing = prior + source
        current = smoothed
        for step in range(ITERS):
            current = (forcing + off_terms(pad_space(current), diffusion, advection)) / diagonal
        smoothed = current
    prior = jnp.roll(smoothed, 1, axis=0)
    applied = diagonal * smoothed - off_terms(pad_space(smoothed), diffusion, advection)
    residual = source + prior - applied
    return smoothed, residual
```

```python
import functools

import jax
import jax.numpy as jnp
from jax import lax
from jax.experimental import pallas as pl
from jax.experimental.pallas import tpu as pltpu
from jax.sharding import PartitionSpec as P

SWEEPS = 2
ITERS = 4
HALO = ITERS
MESH = pl.DeviceIdType.MESH


def cuts(edges):
    return list(zip(edges[:-1], edges[1:]))


def plan(planes, step):
    arrive = list(range(0, planes, step)) + [planes]
    ready = lambda edges: [e if e == planes else max(e - (ITERS - 1), 0) for e in edges]
    split = lambda edges, most: sorted({c for a, b in cuts(edges) for c in list(range(a, b, most)) + [b]})
    first = cuts(arrive)
    second = cuts(split(sorted(set(ready(arrive))), step))
    edges = [0] + [b for _, b in second]
    third = cuts(split(sorted(set(ready(edges))), 2))
    return first, second, third


def kernel(planes, steps, sends, initial, source, diffusion, advection, smoothed, residual,
           v0, v1, v2, v3, s1, s2, src, p1, p2, p3, spread, upwind,
           low_z, high_z, low_x, high_x, low_y, high_y, inverse, diagonal, forced, left,
           load_sem, out_sem, send1, recv1, send2, recv2, send3, recv3, hsend, hrecv):
    first, second, third = sends
    time, side = lax.axis_index("tm"), lax.axis_index("space")
    after, before = lax.rem(time + 1, steps), lax.rem(time + steps - 1, steps)
    other = 1 - side
    rows, lanes = v0.shape[1], v0.shape[2]

    def begin(lo, hi, who=side):
        return who * (HALO + lo) + (1 - who) * (HALO + planes - hi)

    def span(lo, hi, who=side):
        return pl.ds(begin(lo, hi, who), hi - lo)

    def grid_span(lo, hi):
        return pl.ds(begin(lo, hi) - HALO, hi - lo)

    barrier = pltpu.get_barrier_semaphore()
    for peer in ((after, side), (before, side), (time, other)):
        pl.semaphore_signal(barrier, inc=1, device_id=peer, device_id_type=MESH)

    inner = pl.ds(HALO, planes)
    loads = [
        pltpu.make_async_copy(diffusion, spread.at[inner], load_sem.at[0]),
        pltpu.make_async_copy(advection, upwind.at[:, inner], load_sem.at[1]),
        pltpu.make_async_copy(source.at[0], src.at[inner], load_sem.at[2]),
        pltpu.make_async_copy(initial.at[0], v0.at[inner], load_sem.at[3]),
    ]
    for load in loads:
        load.start()

    edge = begin(planes, planes + 1)
    for field in (v0, v1, v2, v3, s1, s2):
        field[edge] = jnp.zeros((rows, lanes), jnp.float32)

    def forward(source_ref, target_ref, send, recv):
        return pltpu.make_async_remote_copy(
            src_ref=source_ref, dst_ref=target_ref, send_sem=send, recv_sem=recv,
            device_id=(after, side), device_id_type=MESH)

    def across(source_ref, target_ref, n):
        return pltpu.make_async_remote_copy(
            src_ref=source_ref, dst_ref=target_ref, send_sem=hsend.at[n], recv_sem=hrecv.at[n],
            device_id=(time, other), device_id_type=MESH)

    def rim(field, width, n):
        return across(field.at[span(0, width)], field.at[span(-width, 0, other)], n)

    near = HALO - 1
    sent1 = [
        forward(initial.at[0, grid_span(lo, hi)], p1.at[span(lo, hi)], send1.at[k], recv1.at[k])
        for k, (lo, hi) in enumerate(first)
    ]
    sent2 = [
        forward(s1.at[span(lo, hi)], p2.at[span(lo, hi)], send2.at[k], recv2.at[k])
        for k, (lo, hi) in enumerate(second)
    ]
    sent3 = [
        forward(s2.at[span(lo, hi)], p3.at[span(lo, hi)], send3.at[k], recv3.at[k])
        for k, (lo, hi) in enumerate(third)
    ]
    rims = [
        across(diffusion.at[grid_span(0, near)], spread.at[span(-near, 0, other)], 0),
        across(advection.at[:, grid_span(0, near)], upwind.at[:, span(-near, 0, other)], 1),
        across(source.at[0, grid_span(0, near)], src.at[span(-near, 0, other)], 2),
        across(initial.at[0, grid_span(0, HALO)], v0.at[span(-HALO, 0, other)], 3),
    ]
    rim_p1, rim_s1, rim_p2, rim_s2 = rim(p1, near, 4), rim(s1, HALO, 5), rim(p2, near, 6), rim(s2, 1, 7)

    pl.semaphore_wait(barrier, 3)
    sent1[0].start()
    for copy in rims:
        copy.start()
    for copy in sent1[1:]:
        copy.start()

    def each(lo, hi, body):
        if hi > lo:
            start = begin(lo, hi)

            def one(k, carry):
                body(start + k)
                return carry

            lax.fori_loop(0, hi - lo, one, 0)

    def coefficients(i):
        d = spread[i]
        ax, ay, az = upwind[0, i], upwind[1, i], upwind[2, i]
        main = 1.0 + 6.0 * d + (ax + ay + az)
        inv = 1.0 / main
        row = lax.broadcasted_iota(jnp.int32, (rows, lanes), 0)
        lane = lax.broadcasted_iota(jnp.int32, (rows, lanes), 1)
        even = d * inv
        high_z[i] = even
        low_z[i] = (d + az) * inv
        high_x[i] = jnp.where(row == rows - 1, 0.0, even)
        low_x[i] = jnp.where(row == 0, 0.0, (d + ax) * inv)
        high_y[i] = jnp.where(lane == lanes - 1, 0.0, even)
        low_y[i] = jnp.where(lane == 0, 0.0, (d + ay) * inv)
        inverse[i] = inv
        diagonal[i] = main

    def neighbours(v, i):
        here = v[i]
        total = low_z[i] * v[i - 1] + high_z[i] * v[i + 1]
        total += low_x[i] * pltpu.roll(here, 1, 0) + high_x[i] * pltpu.roll(here, rows - 1, 0)
        return total + (low_y[i] * pltpu.roll(here, 1, 1) + high_y[i] * pltpu.roll(here, lanes - 1, 1))

    def sweep(start, target, prior, arrivals, ranges, rim_prior, on_ready):
        levels = [start, v1, v2, v3, target]
        reached = [-near] + [-(ITERS - n) for n in range(1, ITERS + 1)]
        rimmed = False
        for k, (lo, hi) in enumerate(ranges):
            arrivals[k].wait_recv()
            if hi < near:
                continue
            if not rimmed:
                rim_prior.start()
                rim_prior.wait_recv()
                rimmed = True
            goal = hi

            def force(i):
                forced[i] = (prior[i] + src[i]) * inverse[i]

            each(reached[0], goal, force)
            reached[0] = goal
            for n in range(1, ITERS + 1):
                goal = hi if hi == planes else hi - (n - 1)

                def iterate(i, n=n):
                    levels[n][i] = forced[i] + neighbours(levels[n - 1], i)

                each(reached[n], goal, iterate)
                reached[n] = max(reached[n], goal)
            on_ready(reached[ITERS])

    for n in (0, 1):
        loads[n].wait()
        rims[n].wait_recv()
    each(-near, planes, coefficients)
    for n in (2, 3):
        loads[n].wait()
        rims[n].wait_recv()

    issued = {"s1": 0, "s2": 0, "rim": set()}

    def issue(name, copies, ranges, ready, extra=None):
        while issued[name] < len(ranges) and ranges[issued[name]][1] <= ready:
            copies[issued[name]].start()
            if extra is not None:
                extra[issued[name]].start()
            issued[name] += 1

    def first_ready(ready):
        if ready >= HALO and "s1" not in issued["rim"]:
            issued["rim"].add("s1")
            rim_s1.start()
        issue("s1", sent2, second, ready)

    outs = [
        pltpu.make_async_copy(s2.at[span(lo, hi)], smoothed.at[0, grid_span(lo, hi)], out_sem.at[0, k])
        for k, (lo, hi) in enumerate(third)
    ]

    def second_ready(ready):
        if ready >= 1 and "s2" not in issued["rim"]:
            issued["rim"].add("s2")
            rim_s2.start()
        issue("s2", sent3, third, ready, outs)

    sweep(v0, s1, p1, sent1, first, rim_p1, first_ready)
    rim_s1.wait_recv()
    sweep(s1, s2, p2, sent2, second, rim_p2, second_ready)
    rim_s2.wait_recv()

    def partial(i):
        left[i] = src[i] - diagonal[i] * (s2[i] - neighbours(s2, i))

    each(0, planes, partial)

    ends = [
        pltpu.make_async_copy(left.at[span(lo, hi)], residual.at[0, grid_span(lo, hi)], out_sem.at[1, k])
        for k, (lo, hi) in enumerate(third)
    ]
    for k, (lo, hi) in enumerate(third):
        sent3[k].wait_recv()

        def finish(i):
            left[i] = left[i] + p3[i]

        each(lo, hi, finish)
        ends[k].start()

    for copy in rims + [rim_p1, rim_s1, rim_p2, rim_s2] + sent1 + sent2 + sent3:
        copy.wait_send()
    for copy in outs + ends:
        copy.wait()


def body(steps, sides, initial, source, diffusion, advection):
    assert sides == 2
    _, planes, rows, lanes = initial.shape
    sends = plan(planes, 4)
    most = max(len(s) for s in sends)
    wide = pltpu.VMEM((planes + 2 * HALO, rows, lanes), jnp.float32)
    triple = pltpu.VMEM((3, planes + 2 * HALO, rows, lanes), jnp.float32)
    dma = pltpu.SemaphoreType.DMA
    pairs = [dma((len(s),)) for s in sends for _ in range(2)]
    result = jax.ShapeDtypeStruct(initial.shape, jnp.float32)
    return pl.pallas_call(
        functools.partial(kernel, planes, steps, sends),
        out_shape=(result, result),
        in_specs=[pl.BlockSpec(memory_space=pl.ANY)] * 4,
        out_specs=(pl.BlockSpec(memory_space=pl.ANY),) * 2,
        scratch_shapes=[wide] * 11 + [triple] + [wide] * 10
        + [dma((4,)), dma((2, most))] + pairs + [dma((8,)), dma((8,))],
        compiler_params=pltpu.CompilerParams(collective_id=0, has_side_effects=True),
        name="smooth",
    )(initial, source, diffusion, advection)


def solution(mesh):
    in_specs = (
        P("tm", "space", None, None),
        P("tm", "space", None, None),
        P("space", None, None),
        P(None, "space", None, None),
    )
    out_specs = (P("tm", "space", None, None), P("tm", "space", None, None))
    run = functools.partial(body, mesh.shape["tm"], mesh.shape["space"])
    return jax.shard_map(run, mesh=mesh, in_specs=in_specs, out_specs=out_specs, check_vma=False)
```

```python
import functools

import jax
import jax.numpy as jnp
from jax import lax
from jax.experimental import pallas as pl
from jax.experimental.pallas import tpu as pltpu
from jax.sharding import PartitionSpec as P

SWEEPS = 2
ITERS = 4
HALO = ITERS
MESH = pl.DeviceIdType.MESH


def cuts(edges):
    return list(zip(edges[:-1], edges[1:]))


def plan(planes, step):
    arrive = list(range(0, planes, step)) + [planes]
    ready = lambda edges: [e if e == planes else max(e - (ITERS - 1), 0) for e in edges]
    split = lambda edges, most: sorted({c for a, b in cuts(edges) for c in list(range(a, b, most)) + [b]})
    first = cuts(arrive)
    second = cuts(split(sorted(set(ready(arrive))), step))
    edges = [0] + [b for _, b in second]
    third = cuts(split(sorted(set(ready(edges))), 2))
    return first, second, third


def kernel(planes, steps, sends, initial, source, diffusion, advection, s2, left, p3,
           v0, v1, v2, v3, s1, src, p1, p2, spread, upwind,
           low_z, high_z, low_x, high_x, low_y, high_y, inverse, diagonal, forced,
           load_sem, send1, recv1, send2, recv2, send3, recv3, hsend, hrecv):
    first, second, third = sends
    time, side = lax.axis_index("tm"), lax.axis_index("space")
    after, before = lax.rem(time + 1, steps), lax.rem(time + steps - 1, steps)
    other = 1 - side
    rows, lanes = v0.shape[1], v0.shape[2]

    def begin(lo, hi, who=side):
        return who * (HALO + lo) + (1 - who) * (HALO + planes - hi)

    def span(lo, hi, who=side):
        return pl.ds(begin(lo, hi, who), hi - lo)

    def grid_span(lo, hi):
        return pl.ds(begin(lo, hi) - HALO, hi - lo)

    barrier = pltpu.get_barrier_semaphore()
    for peer in ((before, side), (time, other)):
        pl.semaphore_signal(barrier, inc=1, device_id=peer, device_id_type=MESH)

    inner = pl.ds(HALO, planes)
    loads = [
        pltpu.make_async_copy(diffusion, spread.at[inner], load_sem.at[0]),
        pltpu.make_async_copy(advection, upwind.at[:, inner], load_sem.at[1]),
        pltpu.make_async_copy(source.at[0], src.at[inner], load_sem.at[2]),
        pltpu.make_async_copy(initial.at[0], v0.at[inner], load_sem.at[3]),
    ]
    for load in loads:
        load.start()

    edge = begin(planes, planes + 1)
    for field in (v0, v1, v2, v3, s1, s2):
        field[edge] = jnp.zeros((rows, lanes), jnp.float32)

    def forward(source_ref, target_ref, send, recv):
        return pltpu.make_async_remote_copy(
            src_ref=source_ref, dst_ref=target_ref, send_sem=send, recv_sem=recv,
            device_id=(after, side), device_id_type=MESH)

    def across(source_ref, target_ref, n):
        return pltpu.make_async_remote_copy(
            src_ref=source_ref, dst_ref=target_ref, send_sem=hsend.at[n], recv_sem=hrecv.at[n],
            device_id=(time, other), device_id_type=MESH)

    def rim(field, width, n):
        return across(field.at[span(0, width)], field.at[span(-width, 0, other)], n)

    near = HALO - 1
    sent1 = [
        forward(initial.at[0, grid_span(lo, hi)], p1.at[span(lo, hi)], send1.at[k], recv1.at[k])
        for k, (lo, hi) in enumerate(first)
    ]
    sent2 = [
        forward(s1.at[span(lo, hi)], p2.at[span(lo, hi)], send2.at[k], recv2.at[k])
        for k, (lo, hi) in enumerate(second)
    ]
    sent3 = [
        forward(s2.at[span(lo, hi)], p3.at[span(lo, hi)], send3.at[k], recv3.at[k])
        for k, (lo, hi) in enumerate(third)
    ]
    rims = [
        across(diffusion.at[grid_span(0, near)], spread.at[span(-near, 0, other)], 0),
        across(advection.at[:, grid_span(0, near)], upwind.at[:, span(-near, 0, other)], 1),
        across(source.at[0, grid_span(0, near)], src.at[span(-near, 0, other)], 2),
        across(initial.at[0, grid_span(0, HALO)], v0.at[span(-HALO, 0, other)], 3),
    ]
    rim_p1, rim_s1, rim_p2, rim_s2 = rim(p1, near, 4), rim(s1, HALO, 5), rim(p2, near, 6), rim(s2, 1, 7)

    pl.semaphore_wait(barrier, 2)
    sent1[0].start()
    for copy in rims:
        copy.start()
    for copy in sent1[1:]:
        copy.start()

    def each(lo, hi, body):
        if hi > lo:
            start = begin(lo, hi)

            def one(k, carry):
                body(start + k)
                return carry

            lax.fori_loop(0, hi - lo, one, 0)

    def coefficients(i):
        d = spread[i]
        ax, ay, az = upwind[0, i], upwind[1, i], upwind[2, i]
        main = 1.0 + 6.0 * d + (ax + ay + az)
        inv = 1.0 / main
        row = lax.broadcasted_iota(jnp.int32, (rows, lanes), 0)
        lane = lax.broadcasted_iota(jnp.int32, (rows, lanes), 1)
        even = d * inv
        high_z[i] = even
        low_z[i] = (d + az) * inv
        high_x[i] = jnp.where(row == rows - 1, 0.0, even)
        low_x[i] = jnp.where(row == 0, 0.0, (d + ax) * inv)
        high_y[i] = jnp.where(lane == lanes - 1, 0.0, even)
        low_y[i] = jnp.where(lane == 0, 0.0, (d + ay) * inv)
        inverse[i] = inv
        diagonal[i] = main

    def neighbours(v, i):
        here = v[i]
        total = low_z[i] * v[i - 1] + high_z[i] * v[i + 1]
        total += low_x[i] * pltpu.roll(here, 1, 0) + high_x[i] * pltpu.roll(here, rows - 1, 0)
        return total + (low_y[i] * pltpu.roll(here, 1, 1) + high_y[i] * pltpu.roll(here, lanes - 1, 1))

    def sweep(start, target, prior, arrivals, ranges, rim_prior, on_ready):
        levels = [start, v1, v2, v3, target]
        reached = [-near] + [-(ITERS - n) for n in range(1, ITERS + 1)]
        rimmed = False
        for k, (lo, hi) in enumerate(ranges):
            arrivals[k].wait_recv()
            if hi < near:
                continue
            if not rimmed:
                rim_prior.start()
                rim_prior.wait_recv()
                rimmed = True
            goal = hi

            def force(i):
                forced[i] = (prior[i] + src[i]) * inverse[i]

            each(reached[0], goal, force)
            reached[0] = goal
            for n in range(1, ITERS + 1):
                goal = hi if hi == planes else hi - (n - 1)

                def iterate(i, n=n):
                    levels[n][i] = forced[i] + neighbours(levels[n - 1], i)

                each(reached[n], goal, iterate)
                reached[n] = max(reached[n], goal)
            on_ready(reached[ITERS])

    for n in (0, 1):
        loads[n].wait()
        rims[n].wait_recv()
    each(-near, planes, coefficients)
    for n in (2, 3):
        loads[n].wait()
        rims[n].wait_recv()

    issued = {"s1": 0, "s2": 0, "rim": set()}

    def issue(name, copies, ranges, ready):
        while issued[name] < len(ranges) and ranges[issued[name]][1] <= ready:
            copies[issued[name]].start()
            issued[name] += 1

    def first_ready(ready):
        if ready >= HALO and "s1" not in issued["rim"]:
            issued["rim"].add("s1")
            rim_s1.start()
        issue("s1", sent2, second, ready)

    def second_ready(ready):
        if ready >= 1 and "s2" not in issued["rim"]:
            issued["rim"].add("s2")
            rim_s2.start()
        issue("s2", sent3, third, ready)

    sweep(v0, s1, p1, sent1, first, rim_p1, first_ready)
    rim_s1.wait_recv()
    sweep(s1, s2, p2, sent2, second, rim_p2, second_ready)
    rim_s2.wait_recv()

    def partial(i):
        left[i] = src[i] - diagonal[i] * (s2[i] - neighbours(s2, i))

    each(0, planes, partial)

    for copy in sent3:
        copy.wait_recv()
    for copy in rims + [rim_p1, rim_s1, rim_p2, rim_s2] + sent1 + sent2 + sent3:
        copy.wait_send()


def finish(planes, step, s2, left, p3, smoothed, residual, total, sem):
    out = pltpu.make_async_copy(s2.at[pl.ds(HALO, planes)], smoothed.at[0], sem.at[0])
    out.start()
    copies = [out]
    for k, lo in enumerate(range(0, planes, step)):
        size = min(step, planes - lo)
        part, wide = pl.ds(lo, size), pl.ds(HALO + lo, size)
        total[part] = left[wide] + p3[wide]
        copies.append(pltpu.make_async_copy(total.at[part], residual.at[0, part], sem.at[1 + k]))
        copies[-1].start()
    for copy in copies:
        copy.wait()


def body(steps, sides, initial, source, diffusion, advection):
    assert sides == 2
    _, planes, rows, lanes = initial.shape
    sends = plan(planes, 4)
    shape = (planes + 2 * HALO, rows, lanes)
    wide = pltpu.VMEM(shape, jnp.float32)
    triple = pltpu.VMEM((3,) + shape, jnp.float32)
    dma = pltpu.SemaphoreType.DMA
    pairs = [dma((len(s),)) for s in sends for _ in range(2)]
    result = jax.ShapeDtypeStruct(initial.shape, jnp.float32)
    vmem = pl.BlockSpec(memory_space=pltpu.VMEM)
    hbm = pl.BlockSpec(memory_space=pltpu.HBM)
    held = pl.pallas_call(
        functools.partial(kernel, planes, steps, sends),
        out_shape=(wide,) * 3,
        in_specs=[hbm] * 4,
        out_specs=(vmem,) * 3,
        scratch_shapes=[wide] * 9 + [triple] + [wide] * 9
        + [dma((4,))] + pairs + [dma((8,)), dma((8,))],
        compiler_params=pltpu.CompilerParams(collective_id=0, has_side_effects=True, vmem_limit_bytes=40 << 20),
        name="smooth",
    )(initial, source, diffusion, advection)
    step = 4
    return pl.pallas_call(
        functools.partial(finish, planes, step),
        out_shape=(result, result),
        in_specs=[vmem] * 3,
        out_specs=(hbm,) * 2,
        scratch_shapes=[pltpu.VMEM((planes, rows, lanes), jnp.float32), dma((1 + -(-planes // step),))],
        compiler_params=pltpu.CompilerParams(vmem_limit_bytes=8 << 20),
        name="finish",
    )(*held)


def solution(mesh):
    in_specs = (
        P("tm", "space", None, None),
        P("tm", "space", None, None),
        P("space", None, None),
        P(None, "space", None, None),
    )
    out_specs = (P("tm", "space", None, None), P("tm", "space", None, None))
    run = functools.partial(body, mesh.shape["tm"], mesh.shape["space"])
    return jax.shard_map(run, mesh=mesh, in_specs=in_specs, out_specs=out_specs, check_vma=False)
```

```python
import functools

import jax
import jax.numpy as jnp
from jax import lax
from jax.experimental import pallas as pl
from jax.experimental.pallas import tpu as pltpu
from jax.sharding import PartitionSpec as P

SWEEPS = 2
ITERS = 4
HALO = ITERS
VMEM_BYTES = 67043328
MESH = pl.DeviceIdType.MESH


def cuts(edges):
    return list(zip(edges[:-1], edges[1:]))


def plan(planes, step):
    arrive = list(range(0, planes, step)) + [planes]
    ready = lambda edges: [e if e == planes else max(e - (ITERS - 1), 0) for e in edges]
    split = lambda edges, most: sorted({c for a, b in cuts(edges) for c in list(range(a, b, most)) + [b]})
    first = cuts(arrive)
    second = cuts(split(sorted(set(ready(arrive))), step))
    edges = [0] + [b for _, b in second]
    third = cuts(split(sorted(set(ready(edges))), 2))
    return first, second, third


def kernel(planes, steps, sends, initial, source, diffusion, advection, s2, left, p3,
           v0, v1, v2, v3, s1, src, p1, p2, spread, upwind,
           low_z, high_z, low_x, high_x, low_y, high_y, inverse, diagonal, forced,
           load_sem, send1, recv1, send2, recv2, send3, recv3, hsend, hrecv):
    first, second, third = sends
    time, side = lax.axis_index("tm"), lax.axis_index("space")
    after, before = lax.rem(time + 1, steps), lax.rem(time + steps - 1, steps)
    other = 1 - side
    rows, lanes = v0.shape[1], v0.shape[2]

    def begin(lo, hi, who=side):
        return who * (HALO + lo) + (1 - who) * (HALO + planes - hi)

    def span(lo, hi, who=side):
        return pl.ds(begin(lo, hi, who), hi - lo)

    def grid_span(lo, hi):
        return pl.ds(begin(lo, hi) - HALO, hi - lo)

    barrier = pltpu.get_barrier_semaphore()
    for peer in ((before, side), (time, other)):
        pl.semaphore_signal(barrier, inc=1, device_id=peer, device_id_type=MESH)

    inner = pl.ds(HALO, planes)
    loads = [
        pltpu.make_async_copy(diffusion, spread.at[inner], load_sem.at[0]),
        pltpu.make_async_copy(advection, upwind.at[:, inner], load_sem.at[1]),
        pltpu.make_async_copy(source.at[0], src.at[inner], load_sem.at[2]),
        pltpu.make_async_copy(initial.at[0], v0.at[inner], load_sem.at[3]),
    ]
    for load in loads:
        load.start()

    edge = begin(planes, planes + 1)
    for field in (v0, v1, v2, v3, s1, s2):
        field[edge] = jnp.zeros((rows, lanes), jnp.float32)

    def forward(source_ref, target_ref, send, recv):
        return pltpu.make_async_remote_copy(
            src_ref=source_ref, dst_ref=target_ref, send_sem=send, recv_sem=recv,
            device_id=(after, side), device_id_type=MESH)

    def across(source_ref, target_ref, n):
        return pltpu.make_async_remote_copy(
            src_ref=source_ref, dst_ref=target_ref, send_sem=hsend.at[n], recv_sem=hrecv.at[n],
            device_id=(time, other), device_id_type=MESH)

    def rim(field, width, n):
        return across(field.at[span(0, width)], field.at[span(-width, 0, other)], n)

    near = HALO - 1
    sent1 = [
        forward(initial.at[0, grid_span(lo, hi)], p1.at[span(lo, hi)], send1.at[k], recv1.at[k])
        for k, (lo, hi) in enumerate(first)
    ]
    sent2 = [
        forward(s1.at[span(lo, hi)], p2.at[span(lo, hi)], send2.at[k], recv2.at[k])
        for k, (lo, hi) in enumerate(second)
    ]
    sent3 = [
        forward(s2.at[span(lo, hi)], p3.at[span(lo, hi)], send3.at[k], recv3.at[k])
        for k, (lo, hi) in enumerate(third)
    ]
    rims = [
        across(diffusion.at[grid_span(0, near)], spread.at[span(-near, 0, other)], 0),
        across(advection.at[:, grid_span(0, near)], upwind.at[:, span(-near, 0, other)], 1),
        across(source.at[0, grid_span(0, near)], src.at[span(-near, 0, other)], 2),
        across(initial.at[0, grid_span(0, HALO)], v0.at[span(-HALO, 0, other)], 3),
    ]
    rim_p1, rim_s1, rim_p2, rim_s2 = rim(p1, near, 4), rim(s1, HALO, 5), rim(p2, near, 6), rim(s2, 1, 7)

    pl.semaphore_wait(barrier, 2)
    sent1[0].start()
    for copy in rims:
        copy.start()
    for copy in sent1[1:]:
        copy.start()

    def each(lo, hi, body):
        if hi > lo:
            start = begin(lo, hi)

            def one(k, carry):
                body(start + k)
                return carry

            lax.fori_loop(0, hi - lo, one, 0)

    def coefficients(i):
        d = spread[i]
        ax, ay, az = upwind[0, i], upwind[1, i], upwind[2, i]
        main = 1.0 + 6.0 * d + (ax + ay + az)
        inv = 1.0 / main
        row = lax.broadcasted_iota(jnp.int32, (rows, lanes), 0)
        lane = lax.broadcasted_iota(jnp.int32, (rows, lanes), 1)
        even = d * inv
        high_z[i] = even
        low_z[i] = (d + az) * inv
        high_x[i] = jnp.where(row == rows - 1, 0.0, even)
        low_x[i] = jnp.where(row == 0, 0.0, (d + ax) * inv)
        high_y[i] = jnp.where(lane == lanes - 1, 0.0, even)
        low_y[i] = jnp.where(lane == 0, 0.0, (d + ay) * inv)
        inverse[i] = inv
        diagonal[i] = main

    def neighbours(v, i):
        here = v[i]
        total = low_z[i] * v[i - 1] + high_z[i] * v[i + 1]
        total += low_x[i] * pltpu.roll(here, 1, 0) + high_x[i] * pltpu.roll(here, rows - 1, 0)
        return total + (low_y[i] * pltpu.roll(here, 1, 1) + high_y[i] * pltpu.roll(here, lanes - 1, 1))

    def sweep(start, target, prior, arrivals, ranges, rim_prior, on_ready):
        levels = [start, v1, v2, v3, target]
        reached = [-near] + [-(ITERS - n) for n in range(1, ITERS + 1)]
        rimmed = False
        for k, (lo, hi) in enumerate(ranges):
            arrivals[k].wait_recv()
            if hi < near:
                continue
            if not rimmed:
                rim_prior.start()
                rim_prior.wait_recv()
                rimmed = True
            goal = hi

            def force(i):
                forced[i] = (prior[i] + src[i]) * inverse[i]

            each(reached[0], goal, force)
            reached[0] = goal
            for n in range(1, ITERS + 1):
                goal = hi if hi == planes else hi - (n - 1)

                def iterate(i, n=n):
                    levels[n][i] = forced[i] + neighbours(levels[n - 1], i)

                each(reached[n], goal, iterate)
                reached[n] = max(reached[n], goal)
            on_ready(reached[ITERS])

    for n in (0, 1):
        loads[n].wait()
        rims[n].wait_recv()
    each(-near, planes, coefficients)
    for n in (2, 3):
        loads[n].wait()
        rims[n].wait_recv()

    issued = {"s1": 0, "s2": 0, "rim": set()}

    def issue(name, copies, ranges, ready):
        while issued[name] < len(ranges) and ranges[issued[name]][1] <= ready:
            copies[issued[name]].start()
            issued[name] += 1

    def first_ready(ready):
        if ready >= HALO and "s1" not in issued["rim"]:
            issued["rim"].add("s1")
            rim_s1.start()
        issue("s1", sent2, second, ready)

    def second_ready(ready):
        if ready >= 1 and "s2" not in issued["rim"]:
            issued["rim"].add("s2")
            rim_s2.start()
        issue("s2", sent3, third, ready)

    sweep(v0, s1, p1, sent1, first, rim_p1, first_ready)
    rim_s1.wait_recv()
    sweep(s1, s2, p2, sent2, second, rim_p2, second_ready)
    rim_s2.wait_recv()

    def partial(i):
        left[i] = src[i] - diagonal[i] * (s2[i] - neighbours(s2, i))

    each(0, planes, partial)

    for copy in sent3:
        copy.wait_recv()
    for copy in rims + [rim_p1, rim_s1, rim_p2, rim_s2] + sent1 + sent2 + sent3:
        copy.wait_send()


def finish(planes, step, s2, left, p3, smoothed, residual, total, sem):
    out = pltpu.make_async_copy(s2.at[pl.ds(HALO, planes)], smoothed.at[0], sem.at[0])
    out.start()
    copies = [out]
    for k, lo in enumerate(range(0, planes, step)):
        size = min(step, planes - lo)
        part, wide = pl.ds(lo, size), pl.ds(HALO + lo, size)
        total[part] = left[wide] + p3[wide]
        copies.append(pltpu.make_async_copy(total.at[part], residual.at[0, part], sem.at[1 + k]))
        copies[-1].start()
    for copy in copies:
        copy.wait()


def body(steps, sides, initial, source, diffusion, advection):
    assert sides == 2
    _, planes, rows, lanes = initial.shape
    sends = plan(planes, 4)
    shape = (planes + 2 * HALO, rows, lanes)
    wide = pltpu.VMEM(shape, jnp.float32)
    triple = pltpu.VMEM((3,) + shape, jnp.float32)
    dma = pltpu.SemaphoreType.DMA
    pairs = [dma((len(s),)) for s in sends for _ in range(2)]
    result = jax.ShapeDtypeStruct(initial.shape, jnp.float32)
    vmem = pl.BlockSpec(memory_space=pltpu.VMEM)
    hbm = pl.BlockSpec(memory_space=pltpu.HBM)
    grant = VMEM_BYTES - (3 * shape[0] + 4) * rows * lanes * 4
    held = pl.pallas_call(
        functools.partial(kernel, planes, steps, sends),
        out_shape=(wide,) * 3,
        in_specs=[hbm] * 4,
        out_specs=(vmem,) * 3,
        scratch_shapes=[wide] * 9 + [triple] + [wide] * 9
        + [dma((4,))] + pairs + [dma((8,)), dma((8,))],
        compiler_params=pltpu.CompilerParams(collective_id=0, has_side_effects=True, vmem_limit_bytes=grant),
        name="smooth",
    )(initial, source, diffusion, advection)
    step = 4
    return pl.pallas_call(
        functools.partial(finish, planes, step),
        out_shape=(result, result),
        in_specs=[vmem] * 3,
        out_specs=(hbm,) * 2,
        scratch_shapes=[pltpu.VMEM((planes, rows, lanes), jnp.float32), dma((1 + -(-planes // step),))],
        compiler_params=pltpu.CompilerParams(vmem_limit_bytes=8 << 20),
        name="finish",
    )(*held)


def solution(mesh):
    in_specs = (
        P("tm", "space", None, None),
        P("tm", "space", None, None),
        P("space", None, None),
        P(None, "space", None, None),
    )
    out_specs = (P("tm", "space", None, None), P("tm", "space", None, None))
    run = functools.partial(body, mesh.shape["tm"], mesh.shape["space"])
    return jax.shard_map(run, mesh=mesh, in_specs=in_specs, out_specs=out_specs, check_vma=False)
```

```python
import functools

import jax
import jax.numpy as jnp
from jax import lax
from jax.experimental import pallas as pl
from jax.experimental.pallas import tpu as pltpu
from jax.sharding import PartitionSpec as P

SWEEPS = 2
ITERS = 4
HALO = ITERS
VMEM_BYTES = 67043328
MESH = pl.DeviceIdType.MESH


def cuts(edges):
    return list(zip(edges[:-1], edges[1:]))


def plan(planes, step):
    arrive = list(range(0, planes, step)) + [planes]
    ready = lambda edges: [e if e == planes else max(e - (ITERS - 1), 0) for e in edges]
    split = lambda edges, most: sorted({c for a, b in cuts(edges) for c in list(range(a, b, most)) + [b]})
    first = cuts(arrive)
    lo, hi = first[-1]
    first = first[:-1] + [(lo, (lo + hi) // 2), ((lo + hi) // 2, hi)]
    second = cuts(split(sorted(set(ready(arrive))), step))
    edges = [0] + [b for _, b in second]
    third = cuts(split(sorted(set(ready(edges))), 2))
    return first, second, third


def kernel(planes, steps, sends, relays, initial, source, diffusion, advection, s2, left, p3,
           v0, v1, v2, v3, s1, src, p1, p2, spread, upwind,
           low_z, high_z, low_x, high_x, low_y, high_y, inverse, diagonal, forced,
           held, load_sem, send1, recv1, send2, recv2, send3, recv3, hsend, hrecv, rsend, rrecv):
    first, second, third = sends
    time, side = lax.axis_index("tm"), lax.axis_index("space")
    after, before = lax.rem(time + 1, steps), lax.rem(time + steps - 1, steps)
    other = 1 - side
    rows, lanes = v0.shape[1], v0.shape[2]

    def begin(lo, hi, who=side):
        return who * (HALO + lo) + (1 - who) * (HALO + planes - hi)

    def span(lo, hi, who=side):
        return pl.ds(begin(lo, hi, who), hi - lo)

    def grid_span(lo, hi):
        return pl.ds(begin(lo, hi) - HALO, hi - lo)

    barrier = pltpu.get_barrier_semaphore()
    for peer in ((before, side), (time, other)):
        pl.semaphore_signal(barrier, inc=1, device_id=peer, device_id_type=MESH)
    last = steps - 1
    greeted = 2
    for stop, _ in relays:
        @pl.when(time == 0)
        def _():
            pl.semaphore_signal(barrier, inc=1, device_id=(stop, side), device_id_type=MESH)

        @pl.when(time == stop)
        def _():
            pl.semaphore_signal(barrier, inc=1, device_id=(last, side), device_id_type=MESH)

        greeted += jnp.where((time == stop) | (time == last), 1, 0)

    inner = pl.ds(HALO, planes)
    loads = [
        pltpu.make_async_copy(diffusion, spread.at[inner], load_sem.at[0]),
        pltpu.make_async_copy(advection, upwind.at[:, inner], load_sem.at[1]),
        pltpu.make_async_copy(source.at[0], src.at[inner], load_sem.at[2]),
        pltpu.make_async_copy(initial.at[0], v0.at[inner], load_sem.at[3]),
    ]
    for load in loads:
        load.start()

    edge = begin(planes, planes + 1)
    for field in (v0, v1, v2, v3, s1, s2):
        field[edge] = jnp.zeros((rows, lanes), jnp.float32)

    def forward(source_ref, target_ref, send, recv):
        return pltpu.make_async_remote_copy(
            src_ref=source_ref, dst_ref=target_ref, send_sem=send, recv_sem=recv,
            device_id=(after, side), device_id_type=MESH)

    def across(source_ref, target_ref, n):
        return pltpu.make_async_remote_copy(
            src_ref=source_ref, dst_ref=target_ref, send_sem=hsend.at[n], recv_sem=hrecv.at[n],
            device_id=(time, other), device_id_type=MESH)

    def rim(field, width, n):
        return across(field.at[span(0, width)], field.at[span(-width, 0, other)], n)

    near = HALO - 1
    sent1 = [
        forward(initial.at[0, grid_span(lo, hi)], p1.at[span(lo, hi)], send1.at[k], recv1.at[k])
        for k, (lo, hi) in enumerate(first)
    ]
    sent2 = [
        forward(s1.at[span(lo, hi)], p2.at[span(lo, hi)], send2.at[k], recv2.at[k])
        for k, (lo, hi) in enumerate(second)
    ]
    sent3 = [
        forward(s2.at[span(lo, hi)], p3.at[span(lo, hi)], send3.at[k], recv3.at[k])
        for k, (lo, hi) in enumerate(third)
    ]
    rims = [
        across(diffusion.at[grid_span(0, near)], spread.at[span(-near, 0, other)], 0),
        across(advection.at[:, grid_span(0, near)], upwind.at[:, span(-near, 0, other)], 1),
        across(source.at[0, grid_span(0, near)], src.at[span(-near, 0, other)], 2),
        across(initial.at[0, grid_span(0, HALO)], v0.at[span(-HALO, 0, other)], 3),
    ]
    rim_p1, rim_s1, rim_p2, rim_s2 = rim(p1, near, 4), rim(s1, HALO, 5), rim(p2, near, 6), rim(s2, 1, 7)

    pl.semaphore_wait(barrier, greeted)
    relayed = {chunk: (n, stop) for n, (stop, chunk) in enumerate(relays)}
    outward, onward = {}, {}
    for chunk, (n, stop) in relayed.items():
        lo, hi = first[chunk]
        room = held.at[n, pl.ds(0, hi - lo)]
        outward[chunk] = pltpu.make_async_remote_copy(
            src_ref=initial.at[0, grid_span(lo, hi)], dst_ref=room, send_sem=send1.at[chunk],
            recv_sem=rrecv.at[n], device_id=(stop, side), device_id_type=MESH)
        onward[chunk] = pltpu.make_async_remote_copy(
            src_ref=room, dst_ref=p1.at[span(lo, hi)], send_sem=rsend.at[n],
            recv_sem=recv1.at[chunk], device_id=(0, side), device_id_type=MESH)

    sent1[0].start()
    for copy in rims:
        copy.start()
    for chunk in relayed:
        @pl.when(time == last)
        def _():
            outward[chunk].start()

    for chunk, copy in enumerate(sent1):
        if chunk in relayed:
            @pl.when(time != last)
            def _():
                copy.start()
        elif chunk > 0:
            copy.start()

    def pass_on():
        for chunk, (n, stop) in relayed.items():
            @pl.when(time == stop)
            def _():
                outward[chunk].wait_recv()
                onward[chunk].start()

    def each(lo, hi, body):
        if hi > lo:
            start = begin(lo, hi)

            def one(k, carry):
                body(start + k)
                return carry

            lax.fori_loop(0, hi - lo, one, 0)

    def coefficients(i):
        d = spread[i]
        ax, ay, az = upwind[0, i], upwind[1, i], upwind[2, i]
        main = 1.0 + 6.0 * d + (ax + ay + az)
        inv = 1.0 / main
        row = lax.broadcasted_iota(jnp.int32, (rows, lanes), 0)
        lane = lax.broadcasted_iota(jnp.int32, (rows, lanes), 1)
        even = d * inv
        high_z[i] = even
        low_z[i] = (d + az) * inv
        high_x[i] = jnp.where(row == rows - 1, 0.0, even)
        low_x[i] = jnp.where(row == 0, 0.0, (d + ax) * inv)
        high_y[i] = jnp.where(lane == lanes - 1, 0.0, even)
        low_y[i] = jnp.where(lane == 0, 0.0, (d + ay) * inv)
        inverse[i] = inv
        diagonal[i] = main

    def neighbours(v, i):
        here = v[i]
        total = low_z[i] * v[i - 1] + high_z[i] * v[i + 1]
        total += low_x[i] * pltpu.roll(here, 1, 0) + high_x[i] * pltpu.roll(here, rows - 1, 0)
        return total + (low_y[i] * pltpu.roll(here, 1, 1) + high_y[i] * pltpu.roll(here, lanes - 1, 1))

    def sweep(start, target, prior, arrivals, ranges, rim_prior, on_ready):
        levels = [start, v1, v2, v3, target]
        reached = [-near] + [-(ITERS - n) for n in range(1, ITERS + 1)]
        rimmed = False
        for k, (lo, hi) in enumerate(ranges):
            arrivals[k].wait_recv()
            if hi < near:
                continue
            if not rimmed:
                rim_prior.start()
                rim_prior.wait_recv()
                rimmed = True
            goal = hi

            def force(i):
                forced[i] = (prior[i] + src[i]) * inverse[i]

            each(reached[0], goal, force)
            reached[0] = goal
            for n in range(1, ITERS + 1):
                goal = hi if hi == planes else hi - (n - 1)

                def iterate(i, n=n):
                    levels[n][i] = forced[i] + neighbours(levels[n - 1], i)

                each(reached[n], goal, iterate)
                reached[n] = max(reached[n], goal)
            on_ready(reached[ITERS])

    for n in (0, 1):
        loads[n].wait()
        rims[n].wait_recv()
    each(-near, planes, coefficients)
    for n in (2, 3):
        loads[n].wait()
        rims[n].wait_recv()

    issued = {"s1": 0, "s2": 0, "rim": set()}

    def issue(name, copies, ranges, ready):
        while issued[name] < len(ranges) and ranges[issued[name]][1] <= ready:
            copies[issued[name]].start()
            issued[name] += 1

    def first_ready(ready):
        if ready >= HALO and "s1" not in issued["rim"]:
            issued["rim"].add("s1")
            rim_s1.start()
        if "relay" not in issued["rim"]:
            issued["rim"].add("relay")
            pass_on()
        issue("s1", sent2, second, ready)

    def second_ready(ready):
        if ready >= 1 and "s2" not in issued["rim"]:
            issued["rim"].add("s2")
            rim_s2.start()
        issue("s2", sent3, third, ready)

    sweep(v0, s1, p1, sent1, first, rim_p1, first_ready)
    rim_s1.wait_recv()
    sweep(s1, s2, p2, sent2, second, rim_p2, second_ready)
    rim_s2.wait_recv()

    def partial(i):
        left[i] = src[i] - diagonal[i] * (s2[i] - neighbours(s2, i))

    each(0, planes, partial)

    for copy in sent3:
        copy.wait_recv()
    for copy in rims + [rim_p1, rim_s1, rim_p2, rim_s2] + sent1 + sent2 + sent3:
        copy.wait_send()
    for chunk, (n, stop) in relayed.items():
        @pl.when(time == stop)
        def _():
            onward[chunk].wait_send()


def finish(planes, step, s2, left, p3, smoothed, residual, total, sem):
    out = pltpu.make_async_copy(s2.at[pl.ds(HALO, planes)], smoothed.at[0], sem.at[0])
    out.start()
    copies = [out]
    for k, lo in enumerate(range(0, planes, step)):
        size = min(step, planes - lo)
        part, wide = pl.ds(lo, size), pl.ds(HALO + lo, size)
        total[part] = left[wide] + p3[wide]
        copies.append(pltpu.make_async_copy(total.at[part], residual.at[0, part], sem.at[1 + k]))
        copies[-1].start()
    for copy in copies:
        copy.wait()


def body(steps, sides, initial, source, diffusion, advection):
    assert sides == 2
    _, planes, rows, lanes = initial.shape
    sends = plan(planes, 4)
    chunks = len(sends[0])
    relays = [(steps // 4 - 1, chunks - 2), (steps - 3, chunks - 1)] if steps >= 8 else []
    most = max(hi - lo for lo, hi in sends[0])
    shape = (planes + 2 * HALO, rows, lanes)
    wide = pltpu.VMEM(shape, jnp.float32)
    triple = pltpu.VMEM((3,) + shape, jnp.float32)
    dma = pltpu.SemaphoreType.DMA
    pairs = [dma((len(s),)) for s in sends for _ in range(2)]
    result = jax.ShapeDtypeStruct(initial.shape, jnp.float32)
    vmem = pl.BlockSpec(memory_space=pltpu.VMEM)
    hbm = pl.BlockSpec(memory_space=pltpu.HBM)
    grant = VMEM_BYTES - (3 * shape[0] + 4) * rows * lanes * 4
    held = pl.pallas_call(
        functools.partial(kernel, planes, steps, sends, relays),
        out_shape=(wide,) * 3,
        in_specs=[hbm] * 4,
        out_specs=(vmem,) * 3,
        scratch_shapes=[wide] * 9 + [triple] + [wide] * 9
        + [pltpu.VMEM((max(len(relays), 1), most, rows, lanes), jnp.float32)]
        + [dma((4,))] + pairs + [dma((8,))] * 2 + [dma((max(len(relays), 1),))] * 2,
        compiler_params=pltpu.CompilerParams(collective_id=0, has_side_effects=True, vmem_limit_bytes=grant),
        name="smooth",
    )(initial, source, diffusion, advection)
    step = 4
    return pl.pallas_call(
        functools.partial(finish, planes, step),
        out_shape=(result, result),
        in_specs=[vmem] * 3,
        out_specs=(hbm,) * 2,
        scratch_shapes=[pltpu.VMEM((planes, rows, lanes), jnp.float32), dma((1 + -(-planes // step),))],
        compiler_params=pltpu.CompilerParams(vmem_limit_bytes=8 << 20),
        name="finish",
    )(*held)


def solution(mesh):
    in_specs = (
        P("tm", "space", None, None),
        P("tm", "space", None, None),
        P("space", None, None),
        P(None, "space", None, None),
    )
    out_specs = (P("tm", "space", None, None), P("tm", "space", None, None))
    run = functools.partial(body, mesh.shape["tm"], mesh.shape["space"])
    return jax.shard_map(run, mesh=mesh, in_specs=in_specs, out_specs=out_specs, check_vma=False)
```

```python
import functools

import jax
import jax.numpy as jnp
from jax import lax
from jax.experimental import pallas as pl
from jax.experimental.pallas import tpu as pltpu
from jax.sharding import PartitionSpec as P

SWEEPS = 2
ITERS = 4
HALO = ITERS
VMEM_BYTES = 67043328
MESH = pl.DeviceIdType.MESH


def cuts(edges):
    return list(zip(edges[:-1], edges[1:]))


def plan(planes, step):
    arrive = list(range(0, planes, step)) + [planes]
    ready = lambda edges: [e if e == planes else max(e - (ITERS - 1), 0) for e in edges]
    split = lambda edges, most: sorted({c for a, b in cuts(edges) for c in list(range(a, b, most)) + [b]})
    first = cuts(arrive)
    lo, hi = first[-1]
    first = first[:-1] + [(lo, hi - 3), (hi - 3, hi)]
    second = cuts(split(sorted(set(ready(arrive))), step))
    edges = [0] + [b for _, b in second]
    third = cuts(split(sorted(set(ready(edges))), 2))
    return first, second, third


def kernel(planes, steps, sends, relays, initial, source, diffusion, advection, s2, left, p3,
           v0, v1, v2, v3, s1, src, p1, p2, spread, upwind,
           low_z, high_z, low_x, high_x, low_y, high_y, inverse, diagonal, forced,
           held, load_sem, send1, recv1, send2, recv2, send3, recv3, hsend, hrecv, rsend, rrecv):
    first, second, third = sends
    time, side = lax.axis_index("tm"), lax.axis_index("space")
    after, before = lax.rem(time + 1, steps), lax.rem(time + steps - 1, steps)
    other = 1 - side
    rows, lanes = v0.shape[1], v0.shape[2]

    def begin(lo, hi, who=side):
        return who * (HALO + lo) + (1 - who) * (HALO + planes - hi)

    def span(lo, hi, who=side):
        return pl.ds(begin(lo, hi, who), hi - lo)

    def grid_span(lo, hi):
        return pl.ds(begin(lo, hi) - HALO, hi - lo)

    barrier = pltpu.get_barrier_semaphore()
    for peer in ((before, side), (time, other)):
        pl.semaphore_signal(barrier, inc=1, device_id=peer, device_id_type=MESH)
    last = steps - 1
    greeted = 2
    for stop, _ in relays:
        @pl.when(time == 0)
        def _():
            pl.semaphore_signal(barrier, inc=1, device_id=(stop, side), device_id_type=MESH)

        @pl.when(time == stop)
        def _():
            pl.semaphore_signal(barrier, inc=1, device_id=(last, side), device_id_type=MESH)

        greeted += jnp.where((time == stop) | (time == last), 1, 0)

    inner = pl.ds(HALO, planes)
    loads = [
        pltpu.make_async_copy(diffusion, spread.at[inner], load_sem.at[0]),
        pltpu.make_async_copy(advection, upwind.at[:, inner], load_sem.at[1]),
        pltpu.make_async_copy(source.at[0], src.at[inner], load_sem.at[2]),
        pltpu.make_async_copy(initial.at[0], v0.at[inner], load_sem.at[3]),
    ]
    for load in loads:
        load.start()

    edge = begin(planes, planes + 1)
    for field in (v0, v1, v2, v3, s1, s2):
        field[edge] = jnp.zeros((rows, lanes), jnp.float32)

    def forward(source_ref, target_ref, send, recv):
        return pltpu.make_async_remote_copy(
            src_ref=source_ref, dst_ref=target_ref, send_sem=send, recv_sem=recv,
            device_id=(after, side), device_id_type=MESH)

    def across(source_ref, target_ref, n):
        return pltpu.make_async_remote_copy(
            src_ref=source_ref, dst_ref=target_ref, send_sem=hsend.at[n], recv_sem=hrecv.at[n],
            device_id=(time, other), device_id_type=MESH)

    def rim(field, width, n):
        return across(field.at[span(0, width)], field.at[span(-width, 0, other)], n)

    near = HALO - 1
    sent1 = [
        forward(initial.at[0, grid_span(lo, hi)], p1.at[span(lo, hi)], send1.at[k], recv1.at[k])
        for k, (lo, hi) in enumerate(first)
    ]
    sent2 = [
        forward(s1.at[span(lo, hi)], p2.at[span(lo, hi)], send2.at[k], recv2.at[k])
        for k, (lo, hi) in enumerate(second)
    ]
    sent3 = [
        forward(s2.at[span(lo, hi)], p3.at[span(lo, hi)], send3.at[k], recv3.at[k])
        for k, (lo, hi) in enumerate(third)
    ]
    rims = [
        across(diffusion.at[grid_span(0, near)], spread.at[span(-near, 0, other)], 0),
        across(advection.at[:, grid_span(0, near)], upwind.at[:, span(-near, 0, other)], 1),
        across(source.at[0, grid_span(0, near)], src.at[span(-near, 0, other)], 2),
        across(initial.at[0, grid_span(0, HALO)], v0.at[span(-HALO, 0, other)], 3),
    ]
    rim_p1, rim_s1, rim_p2, rim_s2 = rim(p1, near, 4), rim(s1, HALO, 5), rim(p2, near, 6), rim(s2, 1, 7)

    pl.semaphore_wait(barrier, greeted)
    relayed = {chunk: (n, stop) for n, (stop, chunk) in enumerate(relays)}
    outward, onward = {}, {}
    for chunk, (n, stop) in relayed.items():
        lo, hi = first[chunk]
        room = held.at[n, pl.ds(0, hi - lo)]
        outward[chunk] = pltpu.make_async_remote_copy(
            src_ref=initial.at[0, grid_span(lo, hi)], dst_ref=room, send_sem=send1.at[chunk],
            recv_sem=rrecv.at[n], device_id=(stop, side), device_id_type=MESH)
        onward[chunk] = pltpu.make_async_remote_copy(
            src_ref=room, dst_ref=p1.at[span(lo, hi)], send_sem=rsend.at[n],
            recv_sem=recv1.at[chunk], device_id=(0, side), device_id_type=MESH)

    sent1[0].start()
    for copy in rims:
        copy.start()
    for chunk in relayed:
        @pl.when(time == last)
        def _():
            outward[chunk].start()

    for chunk, copy in enumerate(sent1):
        if chunk in relayed:
            @pl.when(time != last)
            def _():
                copy.start()
        elif chunk > 0:
            copy.start()

    def pass_on():
        for chunk, (n, stop) in relayed.items():
            @pl.when(time == stop)
            def _():
                outward[chunk].wait_recv()
                onward[chunk].start()

    def each(lo, hi, body):
        if hi > lo:
            start = begin(lo, hi)

            def one(k, carry):
                body(start + k)
                return carry

            lax.fori_loop(0, hi - lo, one, 0)

    def coefficients(i):
        d = spread[i]
        ax, ay, az = upwind[0, i], upwind[1, i], upwind[2, i]
        main = 1.0 + 6.0 * d + (ax + ay + az)
        inv = 1.0 / main
        row = lax.broadcasted_iota(jnp.int32, (rows, lanes), 0)
        lane = lax.broadcasted_iota(jnp.int32, (rows, lanes), 1)
        even = d * inv
        high_z[i] = even
        low_z[i] = (d + az) * inv
        high_x[i] = jnp.where(row == rows - 1, 0.0, even)
        low_x[i] = jnp.where(row == 0, 0.0, (d + ax) * inv)
        high_y[i] = jnp.where(lane == lanes - 1, 0.0, even)
        low_y[i] = jnp.where(lane == 0, 0.0, (d + ay) * inv)
        inverse[i] = inv
        diagonal[i] = main

    def neighbours(v, i):
        here = v[i]
        total = low_z[i] * v[i - 1] + high_z[i] * v[i + 1]
        total += low_x[i] * pltpu.roll(here, 1, 0) + high_x[i] * pltpu.roll(here, rows - 1, 0)
        return total + (low_y[i] * pltpu.roll(here, 1, 1) + high_y[i] * pltpu.roll(here, lanes - 1, 1))

    def sweep(start, target, prior, arrivals, ranges, rim_prior, on_ready):
        levels = [start, v1, v2, v3, target]
        reached = [-near] + [-(ITERS - n) for n in range(1, ITERS + 1)]
        rimmed = False
        for k, (lo, hi) in enumerate(ranges):
            arrivals[k].wait_recv()
            if hi < near:
                continue
            if not rimmed:
                rim_prior.start()
                rim_prior.wait_recv()
                rimmed = True
            goal = hi

            def force(i):
                forced[i] = (prior[i] + src[i]) * inverse[i]

            each(reached[0], goal, force)
            reached[0] = goal
            for n in range(1, ITERS + 1):
                goal = hi if hi == planes else hi - (n - 1)

                def iterate(i, n=n):
                    levels[n][i] = forced[i] + neighbours(levels[n - 1], i)

                each(reached[n], goal, iterate)
                reached[n] = max(reached[n], goal)
            on_ready(reached[ITERS])

    for n in (0, 1):
        loads[n].wait()
        rims[n].wait_recv()
    each(-near, planes, coefficients)
    for n in (2, 3):
        loads[n].wait()
        rims[n].wait_recv()

    issued = {"s1": 0, "s2": 0, "rim": set()}

    def issue(name, copies, ranges, ready):
        while issued[name] < len(ranges) and ranges[issued[name]][1] <= ready:
            copies[issued[name]].start()
            issued[name] += 1

    def first_ready(ready):
        if ready >= HALO and "s1" not in issued["rim"]:
            issued["rim"].add("s1")
            rim_s1.start()
        if "relay" not in issued["rim"]:
            issued["rim"].add("relay")
            pass_on()
        issue("s1", sent2, second, ready)

    def second_ready(ready):
        if ready >= 1 and "s2" not in issued["rim"]:
            issued["rim"].add("s2")
            rim_s2.start()
        issue("s2", sent3, third, ready)

    sweep(v0, s1, p1, sent1, first, rim_p1, first_ready)
    rim_s1.wait_recv()
    sweep(s1, s2, p2, sent2, second, rim_p2, second_ready)
    rim_s2.wait_recv()

    def partial(i):
        left[i] = src[i] - diagonal[i] * (s2[i] - neighbours(s2, i))

    each(0, planes, partial)

    for copy in sent3:
        copy.wait_recv()
    for copy in rims + [rim_p1, rim_s1, rim_p2, rim_s2] + sent1 + sent2 + sent3:
        copy.wait_send()
    for chunk, (n, stop) in relayed.items():
        @pl.when(time == stop)
        def _():
            onward[chunk].wait_send()


def finish(planes, step, s2, left, p3, smoothed, residual, total, sem):
    out = pltpu.make_async_copy(s2.at[pl.ds(HALO, planes)], smoothed.at[0], sem.at[0])
    out.start()
    copies = [out]
    for k, lo in enumerate(range(0, planes, step)):
        size = min(step, planes - lo)
        part, wide = pl.ds(lo, size), pl.ds(HALO + lo, size)
        total[part] = left[wide] + p3[wide]
        copies.append(pltpu.make_async_copy(total.at[part], residual.at[0, part], sem.at[1 + k]))
        copies[-1].start()
    for copy in copies:
        copy.wait()


def body(steps, sides, initial, source, diffusion, advection):
    assert sides == 2
    _, planes, rows, lanes = initial.shape
    sends = plan(planes, 4)
    chunks = len(sends[0])
    relays = [(steps - 2, chunks - 1)] if steps >= 8 else []
    most = max(hi - lo for lo, hi in sends[0])
    shape = (planes + 2 * HALO, rows, lanes)
    wide = pltpu.VMEM(shape, jnp.float32)
    triple = pltpu.VMEM((3,) + shape, jnp.float32)
    dma = pltpu.SemaphoreType.DMA
    pairs = [dma((len(s),)) for s in sends for _ in range(2)]
    result = jax.ShapeDtypeStruct(initial.shape, jnp.float32)
    vmem = pl.BlockSpec(memory_space=pltpu.VMEM)
    hbm = pl.BlockSpec(memory_space=pltpu.HBM)
    grant = VMEM_BYTES - (3 * shape[0] + 4) * rows * lanes * 4
    held = pl.pallas_call(
        functools.partial(kernel, planes, steps, sends, relays),
        out_shape=(wide,) * 3,
        in_specs=[hbm] * 4,
        out_specs=(vmem,) * 3,
        scratch_shapes=[wide] * 9 + [triple] + [wide] * 9
        + [pltpu.VMEM((max(len(relays), 1), most, rows, lanes), jnp.float32)]
        + [dma((4,))] + pairs + [dma((8,))] * 2 + [dma((max(len(relays), 1),))] * 2,
        compiler_params=pltpu.CompilerParams(collective_id=0, has_side_effects=True, vmem_limit_bytes=grant),
        name="smooth",
    )(initial, source, diffusion, advection)
    step = 4
    return pl.pallas_call(
        functools.partial(finish, planes, step),
        out_shape=(result, result),
        in_specs=[vmem] * 3,
        out_specs=(hbm,) * 2,
        scratch_shapes=[pltpu.VMEM((planes, rows, lanes), jnp.float32), dma((1 + -(-planes // step),))],
        compiler_params=pltpu.CompilerParams(vmem_limit_bytes=8 << 20),
        name="finish",
    )(*held)


def solution(mesh):
    in_specs = (
        P("tm", "space", None, None),
        P("tm", "space", None, None),
        P("space", None, None),
        P(None, "space", None, None),
    )
    out_specs = (P("tm", "space", None, None), P("tm", "space", None, None))
    run = functools.partial(body, mesh.shape["tm"], mesh.shape["space"])
    return jax.shard_map(run, mesh=mesh, in_specs=in_specs, out_specs=out_specs, check_vma=False)
```

```python
import functools

import jax
import jax.numpy as jnp
from jax import lax
from jax.experimental import pallas as pl
from jax.experimental.pallas import tpu as pltpu
from jax.sharding import PartitionSpec as P

SWEEPS = 2
ITERS = 4
HALO = ITERS
VMEM_BYTES = 67043328
MESH = pl.DeviceIdType.MESH


def cuts(edges):
    return list(zip(edges[:-1], edges[1:]))


def plan(planes, step):
    arrive = list(range(0, planes, step)) + [planes]
    ready = lambda edges: [e if e == planes else max(e - (ITERS - 1), 0) for e in edges]
    split = lambda edges, most: sorted({c for a, b in cuts(edges) for c in list(range(a, b, most)) + [b]})
    first = cuts(arrive)
    second = cuts(split(sorted(set(ready(arrive))), step))
    edges = [0] + [b for _, b in second]
    third = cuts(split(sorted(set(ready(edges))), 2))
    return first, second, third


def kernel(planes, steps, sends, initial, source, diffusion, advection, s2, left, p3,
           v0, v1, v2, v3, s1, src, p1, p2, spread, upwind,
           low_z, high_z, low_x, high_x, low_y, high_y, inverse, diagonal, forced,
           load_sem, send1, recv1, send2, recv2, send3, recv3, hsend, hrecv):
    first, second, third = sends
    time, side = lax.axis_index("tm"), lax.axis_index("space")
    after, before = lax.rem(time + 1, steps), lax.rem(time + steps - 1, steps)
    other = 1 - side
    rows, lanes = v0.shape[1], v0.shape[2]

    def begin(lo, hi, who=side):
        return who * (HALO + lo) + (1 - who) * (HALO + planes - hi)

    def span(lo, hi, who=side):
        return pl.ds(begin(lo, hi, who), hi - lo)

    def grid_span(lo, hi):
        return pl.ds(begin(lo, hi) - HALO, hi - lo)

    barrier = pltpu.get_barrier_semaphore()
    for peer in ((before, side), (time, other)):
        pl.semaphore_signal(barrier, inc=1, device_id=peer, device_id_type=MESH)

    inner = pl.ds(HALO, planes)
    loads = [
        pltpu.make_async_copy(diffusion, spread.at[inner], load_sem.at[0]),
        pltpu.make_async_copy(advection, upwind.at[:, inner], load_sem.at[1]),
        pltpu.make_async_copy(source.at[0], src.at[inner], load_sem.at[2]),
        pltpu.make_async_copy(initial.at[0], v0.at[inner], load_sem.at[3]),
    ]
    for load in loads[::-1]:
        load.start()

    edge = begin(planes, planes + 1)
    for field in (v0, v1, v2, v3, s1, s2):
        field[edge] = jnp.zeros((rows, lanes), jnp.float32)

    def forward(source_ref, target_ref, send, recv):
        return pltpu.make_async_remote_copy(
            src_ref=source_ref, dst_ref=target_ref, send_sem=send, recv_sem=recv,
            device_id=(after, side), device_id_type=MESH)

    def across(source_ref, target_ref, n):
        return pltpu.make_async_remote_copy(
            src_ref=source_ref, dst_ref=target_ref, send_sem=hsend.at[n], recv_sem=hrecv.at[n],
            device_id=(time, other), device_id_type=MESH)

    def rim(field, width, n):
        return across(field.at[span(0, width)], field.at[span(-width, 0, other)], n)

    near = HALO - 1
    sent1 = [
        forward(v0.at[span(lo, hi)], p1.at[span(lo, hi)], send1.at[k], recv1.at[k])
        for k, (lo, hi) in enumerate(first)
    ]
    sent2 = [
        forward(s1.at[span(lo, hi)], p2.at[span(lo, hi)], send2.at[k], recv2.at[k])
        for k, (lo, hi) in enumerate(second)
    ]
    sent3 = [
        forward(s2.at[span(lo, hi)], p3.at[span(lo, hi)], send3.at[k], recv3.at[k])
        for k, (lo, hi) in enumerate(third)
    ]
    rims = [
        across(diffusion.at[grid_span(0, near)], spread.at[span(-near, 0, other)], 0),
        across(advection.at[:, grid_span(0, near)], upwind.at[:, span(-near, 0, other)], 1),
        across(source.at[0, grid_span(0, near)], src.at[span(-near, 0, other)], 2),
        across(initial.at[0, grid_span(0, HALO)], v0.at[span(-HALO, 0, other)], 3),
    ]
    rim_p1, rim_s1, rim_p2, rim_s2 = rim(p1, near, 4), rim(s1, HALO, 5), rim(p2, near, 6), rim(s2, 1, 7)

    pl.semaphore_wait(barrier, 2)
    loads[3].wait()
    sent1[0].start()
    for copy in rims:
        copy.start()
    for copy in sent1[1:]:
        copy.start()

    def each(lo, hi, body):
        if hi > lo:
            start = begin(lo, hi)

            def one(k, carry):
                body(start + k)
                return carry

            lax.fori_loop(0, hi - lo, one, 0)

    def coefficients(i):
        d = spread[i]
        ax, ay, az = upwind[0, i], upwind[1, i], upwind[2, i]
        main = 1.0 + 6.0 * d + (ax + ay + az)
        inv = 1.0 / main
        row = lax.broadcasted_iota(jnp.int32, (rows, lanes), 0)
        lane = lax.broadcasted_iota(jnp.int32, (rows, lanes), 1)
        even = d * inv
        high_z[i] = even
        low_z[i] = (d + az) * inv
        high_x[i] = jnp.where(row == rows - 1, 0.0, even)
        low_x[i] = jnp.where(row == 0, 0.0, (d + ax) * inv)
        high_y[i] = jnp.where(lane == lanes - 1, 0.0, even)
        low_y[i] = jnp.where(lane == 0, 0.0, (d + ay) * inv)
        inverse[i] = inv
        diagonal[i] = main

    def neighbours(v, i):
        here = v[i]
        total = low_z[i] * v[i - 1] + high_z[i] * v[i + 1]
        total += low_x[i] * pltpu.roll(here, 1, 0) + high_x[i] * pltpu.roll(here, rows - 1, 0)
        return total + (low_y[i] * pltpu.roll(here, 1, 1) + high_y[i] * pltpu.roll(here, lanes - 1, 1))

    def sweep(start, target, prior, arrivals, ranges, rim_prior, on_ready):
        levels = [start, v1, v2, v3, target]
        reached = [-near] + [-(ITERS - n) for n in range(1, ITERS + 1)]
        rimmed = False
        for k, (lo, hi) in enumerate(ranges):
            arrivals[k].wait_recv()
            if hi < near:
                continue
            if not rimmed:
                rim_prior.start()
                rim_prior.wait_recv()
                rimmed = True
            goal = hi

            def force(i):
                forced[i] = (prior[i] + src[i]) * inverse[i]

            each(reached[0], goal, force)
            reached[0] = goal
            for n in range(1, ITERS + 1):
                goal = hi if hi == planes else hi - (n - 1)

                def iterate(i, n=n):
                    levels[n][i] = forced[i] + neighbours(levels[n - 1], i)

                each(reached[n], goal, iterate)
                reached[n] = max(reached[n], goal)
            on_ready(reached[ITERS])

    for n in (0, 1):
        loads[n].wait()
        rims[n].wait_recv()
    each(-near, planes, coefficients)
    loads[2].wait()
    for n in (2, 3):
        rims[n].wait_recv()

    issued = {"s1": 0, "s2": 0, "rim": set()}

    def issue(name, copies, ranges, ready):
        while issued[name] < len(ranges) and ranges[issued[name]][1] <= ready:
            copies[issued[name]].start()
            issued[name] += 1

    def first_ready(ready):
        if ready >= HALO and "s1" not in issued["rim"]:
            issued["rim"].add("s1")
            rim_s1.start()
        issue("s1", sent2, second, ready)

    def second_ready(ready):
        if ready >= 1 and "s2" not in issued["rim"]:
            issued["rim"].add("s2")
            rim_s2.start()
        issue("s2", sent3, third, ready)

    sweep(v0, s1, p1, sent1, first, rim_p1, first_ready)
    rim_s1.wait_recv()
    sweep(s1, s2, p2, sent2, second, rim_p2, second_ready)
    rim_s2.wait_recv()

    def partial(i):
        left[i] = src[i] - diagonal[i] * (s2[i] - neighbours(s2, i))

    each(0, planes, partial)

    for copy in sent3:
        copy.wait_recv()
    for copy in rims + [rim_p1, rim_s1, rim_p2, rim_s2] + sent1 + sent2 + sent3:
        copy.wait_send()


def finish(planes, step, s2, left, p3, smoothed, residual, total, sem):
    out = pltpu.make_async_copy(s2.at[pl.ds(HALO, planes)], smoothed.at[0], sem.at[0])
    out.start()
    copies = [out]
    for k, lo in enumerate(range(0, planes, step)):
        size = min(step, planes - lo)
        part, wide = pl.ds(lo, size), pl.ds(HALO + lo, size)
        total[part] = left[wide] + p3[wide]
        copies.append(pltpu.make_async_copy(total.at[part], residual.at[0, part], sem.at[1 + k]))
        copies[-1].start()
    for copy in copies:
        copy.wait()


def body(steps, sides, initial, source, diffusion, advection):
    assert sides == 2
    _, planes, rows, lanes = initial.shape
    sends = plan(planes, 4)
    shape = (planes + 2 * HALO, rows, lanes)
    wide = pltpu.VMEM(shape, jnp.float32)
    triple = pltpu.VMEM((3,) + shape, jnp.float32)
    dma = pltpu.SemaphoreType.DMA
    pairs = [dma((len(s),)) for s in sends for _ in range(2)]
    result = jax.ShapeDtypeStruct(initial.shape, jnp.float32)
    vmem = pl.BlockSpec(memory_space=pltpu.VMEM)
    hbm = pl.BlockSpec(memory_space=pltpu.HBM)
    grant = VMEM_BYTES - (3 * shape[0] + 4) * rows * lanes * 4
    held = pl.pallas_call(
        functools.partial(kernel, planes, steps, sends),
        out_shape=(wide,) * 3,
        in_specs=[hbm] * 4,
        out_specs=(vmem,) * 3,
        scratch_shapes=[wide] * 9 + [triple] + [wide] * 9
        + [dma((4,))] + pairs + [dma((8,)), dma((8,))],
        compiler_params=pltpu.CompilerParams(collective_id=0, has_side_effects=True, vmem_limit_bytes=grant),
        name="smooth",
    )(initial, source, diffusion, advection)
    step = 4
    return pl.pallas_call(
        functools.partial(finish, planes, step),
        out_shape=(result, result),
        in_specs=[vmem] * 3,
        out_specs=(hbm,) * 2,
        scratch_shapes=[pltpu.VMEM((planes, rows, lanes), jnp.float32), dma((1 + -(-planes // step),))],
        compiler_params=pltpu.CompilerParams(vmem_limit_bytes=8 << 20),
        name="finish",
    )(*held)


def solution(mesh):
    in_specs = (
        P("tm", "space", None, None),
        P("tm", "space", None, None),
        P("space", None, None),
        P(None, "space", None, None),
    )
    out_specs = (P("tm", "space", None, None), P("tm", "space", None, None))
    run = functools.partial(body, mesh.shape["tm"], mesh.shape["space"])
    return jax.shard_map(run, mesh=mesh, in_specs=in_specs, out_specs=out_specs, check_vma=False)
```
